32 devices in a mesh: seq: 8 (over y, x, core), exp: 4 (over z).
Axes of the slice: x: 2, y: 2, z: 4, core: 2. Of those that a mesh axis runs over, the one named last changes fastest.
Arguments:
- queries: bfloat16 [8, 512, 512], P(None, 'seq', 'exp'), may hold values from -5 to 5
- keys: bfloat16 [8, 512, 512], P(None, 'seq', 'exp'), may hold values from -5 to 5
- values: bfloat16 [8, 512, 512], P(None, 'seq', 'exp'), may hold values from -170 to 170
- seg_ids: int32 [8, 512], replicated, may hold values from 0 to 3, as said below
- norm_gain: float32 [512], replicated, may hold values from 0.25 to 1.75
- router_w: bfloat16 [512, 16], replicated, may hold values from -0.25 to 0.25
- expert_ids: int32 [512, 8, 1, 2], P(('seq', 'exp')), may hold values from 0 to 15, all different within a row; in each aligned block of 128 rows (0 to 127, 128 to 255, ..., all dimensions but the last counted through in order) at most 32 rows name the same one
- w_in: bfloat16 [16, 512, 1024], P('exp'), may hold values from -0.25 to 0.25
- w_out: bfloat16 [16, 1024, 512], P('exp'), may hold values from -0.1875 to 0.1875
Outputs:
- normed: bfloat16 [8, 512, 512], P(None, ('seq', 'exp'))
- expert_mix: bfloat16 [8, 512, 512], P(None, ('seq', 'exp'))
The draws below stay inside these ranges and needn't reach their ends.
Inputs may be any that keep to these rules, and one draw needn't show every extreme that they name: `seg_ids`: in each sequence the numbers start at 0, never fall, and rise by one at each of 3 document starts; every start lies at an even position after the middle of the sequence. `expert_ids`: the 2 experts of a sub-token differ. Among the rows of one device (its 16 positions, all sequences, all sub-tokens) no expert is named more than 32 times; in every draw some device names some expert exactly 32 times.
All inputs are finite; a program needn't handle non-finite values.
Results may differ from the reference program's by a relative error of at most 0.015.
Values may be sent and summed in bfloat16 or wider, within the bound.
A program may use at most 128 MiB of HBM per device.

```python
import math
import jax
import jax.numpy as jnp
import numpy as np
from jax import lax

HD = 128
HEADS = 4
HF = 512
SUB = 512
SUBS = 1
EXPERTS = 16
FFH = 1024
TOPK = 2
CAP = 32
DOCS = 4
SEQS = 8
TOK_DEV = 16
SEQ_LEN = 512
N_SEQ = 8


def drawn_pair(key):
    shape = (SEQS, SEQ_LEN, HF)
    first = jnp.clip(jax.random.normal(jax.random.fold_in(key, 101), shape, jnp.float32), -5.0, 5.0)
    second = jnp.clip(jax.random.normal(jax.random.fold_in(key, 102), shape, jnp.float32), -5.0, 5.0)
    return (first, second)


def draw_queries(key, part):
    return drawn_pair(key)[0].astype(jnp.bfloat16)


def draw_keys(key, part):
    return drawn_pair(key)[1].astype(jnp.bfloat16)


def draw_values(key, part):
    shape = (SEQS, SEQ_LEN, HF)
    head_of = (jnp.arange(HF) // HD).astype(jnp.float32)
    exponent = head_of / max(HEADS - 1, 1)
    base = jnp.clip(jax.random.normal(jax.random.fold_in(key, 201), shape, jnp.float32), -4.0, 4.0)
    drawn = base * (3.0 ** exponent)[None, None, :]
    return drawn.astype(jnp.bfloat16)


def draw_seg_ids(key, part):
    stacked_rows = []
    for sequence in range(SEQS):
        picked = jax.random.permutation(jax.random.fold_in(key, 31 + sequence), SEQ_LEN // 4 - 1)[:DOCS - 1]
        bounds = 2 * (picked.astype(jnp.int32) + SEQ_LEN // 4 + 1)
        positions = jnp.arange(SEQ_LEN, dtype=jnp.int32)
        stacked_rows.append(jnp.sum((positions[:, None] >= bounds[None, :]).astype(jnp.int32), axis=1))
    return jnp.stack(stacked_rows).astype(jnp.int32)


def level_of(key, extent, shards, least, largest):
    def one(axis_at, blocks):
        draws = jax.random.uniform(jax.random.fold_in(jax.random.fold_in(key, 6), axis_at), (blocks,), jnp.float32, least / len(shards), largest / len(shards))
        return jnp.repeat(jnp.exp(draws), extent[axis_at] // blocks).reshape((-1,) + (1,) * (len(extent) - axis_at - 1))

    level = one(*shards[0])
    for cut in shards[1:]:
        level = level * one(*cut)
    return level


def shared_out(stream_key, own, number, rows, amount, top, reach, lean):
    order = jax.random.permutation(stream_key, amount)
    heavy_load, usual = portions_of(amount, rows * top, reach, lean, True), portions_of(amount, rows * top, reach, lean, False)
    places = jnp.arange(amount)

    def named(lengths, offset_by):
        used = int((lengths > 0).sum())
        fixed = max(1, used // 4)
        passed = fixed + (places - fixed + offset_by * (used - fixed)) % max(1, amount - fixed)
        return jnp.zeros((amount,), jnp.int32).at[order[jnp.where(places < fixed, places, passed)]].set(jnp.asarray(lengths, jnp.int32))

    lengths = jnp.where(number % 4 == 0, named(heavy_load, number // 4), named(usual, number - number // 4 - 1))
    mixed = jax.random.permutation(jax.random.fold_in(own, 3), amount)
    source_of, receiver = mixed[0:amount // 2 * 2:2], mixed[1:amount // 2 * 2:2]
    margin = jnp.minimum(lengths[source_of] - 1, reach - lengths[receiver]) // 2
    margin = jnp.where((source_of == order[0]) | (receiver == order[0]) | (lengths[receiver] == 0), 0, jnp.maximum(margin, 0))
    passed = jax.random.randint(jax.random.fold_in(own, 4), (amount // 2,), 0, 1 << 20) % (margin + 1)
    lengths = lengths.at[source_of].add(-passed).at[receiver].add(passed)
    labels = jnp.searchsorted(jnp.cumsum(lengths), jnp.arange(rows * top), side="right").astype(jnp.int32)
    grid = labels.reshape(top, rows).T
    grid = grid[jax.random.permutation(jax.random.fold_in(own, 1), rows)]
    offset_by = jax.random.randint(jax.random.fold_in(own, 2), (rows, 1), 0, top)
    return jnp.take_along_axis(grid, (jnp.arange(top)[None, :] + offset_by) % top, axis=1)


def portions_of(amount, total, most, slope, full):
    weights = [(1 << 20) // math.isqrt(grade ** slope) + 1 for grade in range(1, amount + 1)]
    largest = most if full else min(most, max(-(-total // amount), total * weights[0] // sum(weights)))
    least = 1 if total - largest >= amount - 1 else 0
    given, rest = [largest] + [least] * (amount - 1), total - largest - least * (amount - 1)
    while rest > 0:
        candidates = [i for i in range(1, amount) if given[i] < largest] or [i for i in range(1, amount) if given[i] < most]
        mass, left = sum([weights[i] for i in candidates]), rest
        for i in candidates:
            more = min(most - given[i], max(1, left * weights[i] // mass), rest)
            given[i] = given[i] + more
            rest = rest - more
    return np.array(given)


def bell_draw(rng, shape, deviation, most, pieces=(), kind=jnp.bfloat16):
    values = deviation * jax.random.normal(rng, shape, jnp.float32)
    if pieces:
        values = values * level_of(rng, shape, pieces, -0.22, 0.18)
    return jnp.clip(values, -most, most).astype(kind)


def setup_inputs(seed: int = 0) -> dict:
    key_list = jax.random.split(jax.random.key(seed), 10)
    queries = draw_queries(jax.random.fold_in(key_list[9], 71), 0)
    keys = draw_keys(jax.random.fold_in(key_list[9], 71), 0)
    values = draw_values(jax.random.fold_in(key_list[9], 71), 0)
    seg_ids = draw_seg_ids(jax.random.fold_in(key_list[9], 71), 0)
    norm_gain = jnp.clip(1.0 + 0.15 * jax.random.normal(key_list[4], (HF,), jnp.float32), 0.25, 1.75)
    router_w = bell_draw(key_list[5], (SUB, EXPERTS), SUB ** -0.5, 0.25)
    expert_ids_keys = jax.random.split(jax.random.fold_in(key_list[6], 1), SEQ_LEN * SEQS * SUBS // (TOK_DEV * SEQS * SUBS))
    expert_ids_turns = jax.random.permutation(jax.random.fold_in(key_list[6], 3), SEQ_LEN * SEQS * SUBS // (TOK_DEV * SEQS * SUBS))
    expert_ids = jax.vmap(lambda own, number: shared_out(jax.random.fold_in(key_list[6], 2), own, number, TOK_DEV * SEQS * SUBS, EXPERTS, TOPK, CAP, 2))(expert_ids_keys, expert_ids_turns).reshape((SEQ_LEN, SEQS, SUBS, TOPK))
    w_in = bell_draw(key_list[7], (EXPERTS, SUB, FFH), SUB ** -0.5, 0.25, ((0, 4),))
    w_out = bell_draw(key_list[8], (EXPERTS, FFH, SUB), FFH ** -0.5, 0.1875, ((0, 4),))
    return dict(queries=queries, keys=keys, values=values, seg_ids=seg_ids, norm_gain=norm_gain, router_w=router_w, expert_ids=expert_ids, w_in=w_in, w_out=w_out)


NEG = -1e+30

def update(running, query_slice, key_slice, value_slice, query_pos, query_seg, key_pos, key_seg, score_scale):
    maxima, totals, running_total = running
    attention_scores = jnp.einsum('uio,umo->uim', query_slice.astype(jnp.float32), key_slice.astype(jnp.float32)) * score_scale
    visible = (key_pos[None, :] <= query_pos[:, None])[None] & (key_seg[:, None, :] == query_seg[:, :, None])
    highest = lax.optimization_barrier(jnp.max(jnp.where(visible, attention_scores, NEG), axis=-1))
    new_max = jnp.maximum(maxima, highest)
    weights = jnp.where(visible, jnp.exp(attention_scores - new_max[..., None]), 0.0)
    rescale_factor = jnp.exp(maxima - new_max)
    totals = totals * rescale_factor + lax.optimization_barrier(jnp.sum(weights, axis=-1))
    rounded_result = weights.astype(jnp.bfloat16)
    running_total = running_total * rescale_factor[..., None] + jnp.einsum('uie,uec->uic', rounded_result.astype(jnp.float32), value_slice.astype(jnp.float32))
    return (new_max, totals, running_total)

def reference(queries, keys, values, seg_ids, norm_gain, router_w, expert_ids, w_in, w_out):
    local_len = SEQ_LEN // N_SEQ
    score_scale = HD ** (-0.5)

    def one_head(head):
        head_queries = lax.dynamic_slice_in_dim(queries, head * HD, HD, 2)
        head_keys = lax.dynamic_slice_in_dim(keys, head * HD, HD, 2)
        head_values = lax.dynamic_slice_in_dim(values, head * HD, HD, 2)

        def one_block(block_index):
            query_first = block_index * local_len
            query_slice = lax.dynamic_slice_in_dim(head_queries, query_first, local_len, 1)
            query_pos = query_first + jnp.arange(local_len, dtype=jnp.int32)
            query_seg = lax.dynamic_slice_in_dim(seg_ids, query_first, local_len, 1)
            initial = (jnp.full((SEQS, local_len), NEG, jnp.float32), jnp.zeros((SEQS, local_len), jnp.float32), jnp.zeros((SEQS, local_len, HD), jnp.float32))

            def over_keys(running, key_index):
                key_first = key_index * local_len
                key_slice = lax.dynamic_slice_in_dim(head_keys, key_first, local_len, 1)
                value_slice = lax.dynamic_slice_in_dim(head_values, key_first, local_len, 1)
                key_seg = lax.dynamic_slice_in_dim(seg_ids, key_first, local_len, 1)
                key_pos = key_first + jnp.arange(local_len, dtype=jnp.int32)
                needed = (key_first <= query_first + local_len - 1) & jnp.any(key_seg[:, -1] >= query_seg[:, 0])
                running = lax.cond(needed, lambda state: update(state, query_slice, key_slice, value_slice, query_pos, query_seg, key_pos, key_seg, score_scale), lambda state: state, running)
                return (running, None)
            final, unused = lax.scan(over_keys, initial, jnp.arange(N_SEQ, dtype=jnp.int32))
            return (final[2] / final[1][..., None]).astype(jnp.bfloat16)
        blocks = lax.map(one_block, jnp.arange(N_SEQ, dtype=jnp.int32))
        return blocks.transpose(1, 0, 2, 3).reshape(SEQS, SEQ_LEN, HD)
    heads = lax.map(one_head, jnp.arange(HEADS, dtype=jnp.int32))
    attended = heads.transpose(1, 2, 0, 3).reshape(SEQS, SEQ_LEN, HF)
    values32 = attended.astype(jnp.float32)
    spread = jnp.sqrt(lax.optimization_barrier(jnp.mean(values32 * values32, axis=-1, keepdims=True)) + 1e-06)
    normed = (values32 / spread * norm_gain).astype(jnp.bfloat16)
    sub_rows = normed.reshape(SEQS, SEQ_LEN, SUBS, SUB).transpose(1, 0, 2, 3).reshape(-1, SUB)
    picks = expert_ids.reshape(-1, TOPK)
    logits = jnp.dot(sub_rows, router_w, preferred_element_type=jnp.float32)
    chosen = jnp.take_along_axis(logits, picks, axis=1)
    sigmas = jax.nn.sigmoid(chosen)
    gates = sigmas / lax.optimization_barrier(jnp.sum(sigmas, axis=1, keepdims=True))
    targets = picks.reshape(-1).astype(jnp.int32)
    assign_count = targets.shape[0]
    order = jnp.argsort(targets, stable=True).astype(jnp.int32)
    counts = jax.ops.segment_sum(jnp.ones_like(targets), targets, num_segments=EXPERTS).astype(jnp.int32)
    block_rows = 512
    padded = ((counts + block_rows - 1) // block_rows * block_rows).astype(jnp.int32)
    padded_start = (jnp.cumsum(padded) - padded).astype(jnp.int32)
    plain_start = (jnp.cumsum(counts) - counts).astype(jnp.int32)
    sorted_targets = targets[order]
    within = jnp.arange(assign_count, dtype=jnp.int32) - plain_start[sorted_targets]
    placed = (padded_start[sorted_targets] + within).astype(jnp.int32)
    block_total = assign_count // block_rows + EXPERTS + 1
    owner = jnp.full((block_total * block_rows,), assign_count, jnp.int32).at[placed].set(order)
    padded_end = padded_start + padded
    block_first = jnp.arange(block_total, dtype=jnp.int32) * block_rows
    block_expert = jnp.minimum(lax.optimization_barrier(jnp.sum((padded_end[None, :] <= block_first[:, None]).astype(jnp.int32), axis=1)), EXPERTS - 1).astype(jnp.int32)

    def run_block(index):
        members = lax.dynamic_slice_in_dim(owner, index * block_rows, block_rows)
        inputs = sub_rows[jnp.minimum(members, assign_count - 1) // TOPK]
        expert = block_expert[index]
        hidden = jax.nn.gelu(jnp.dot(inputs, w_in[expert], preferred_element_type=jnp.float32), approximate=True).astype(jnp.bfloat16)
        return jnp.dot(hidden, w_out[expert], preferred_element_type=jnp.float32).astype(jnp.bfloat16)
    outputs = lax.map(run_block, jnp.arange(block_total, dtype=jnp.int32)).reshape(-1, SUB)
    per_assign = jnp.zeros((assign_count, SUB), jnp.bfloat16).at[owner].set(outputs, mode='drop')
    picked = per_assign.reshape(-1, TOPK, SUB).astype(jnp.float32)
    mixed = lax.optimization_barrier(jnp.sum(gates[:, :, None] * picked, axis=1)).astype(jnp.bfloat16)
    expert_mix = mixed.reshape(SEQ_LEN, SEQS, HF).transpose(1, 0, 2)
    return (normed, expert_mix)
```

```python
import functools

import jax
import jax.numpy as jnp
from jax import lax
from jax.experimental import pallas as pl
from jax.experimental.pallas import tpu as pltpu
from jax.sharding import PartitionSpec as P

HD = 128
SUB = 512
TOPK = 2
CAP = 32


NEG = -1e30


def update(running, query_heads, shaped, query_pos, query_seg, key_pos, key_seg, score_scale):
    maxima, totals, running_total = running
    attention_scores = (
        jnp.einsum("bqhd,bkhd->bhqk", query_heads, shaped[0], preferred_element_type=jnp.float32)
        * score_scale
    )
    visible = (key_pos[None, :] <= query_pos[:, None])[None, None] & (
        key_seg[:, None, None, :] == query_seg[:, None, :, None]
    )
    highest = jnp.max(jnp.where(visible, attention_scores, NEG), axis=-1)
    new_max = jnp.maximum(maxima, highest)
    weights = jnp.where(visible, jnp.exp(attention_scores - new_max[..., None]), 0.0)
    rescale_factor = jnp.exp(maxima - new_max)
    totals = totals * rescale_factor + jnp.sum(weights, axis=-1)
    rounded_result = weights.astype(jnp.bfloat16)
    running_total = running_total * rescale_factor[..., None] + jnp.einsum(
        "bhqk,bkhd->bhqd", rounded_result, shaped[1], preferred_element_type=jnp.float32
    )
    return (new_max, totals, running_total)


def attend_block(
    running, query_heads, block, query_pos, query_seg, seg_ids, key_first, score_scale
):
    row_count = block.shape[2]
    key_pos = key_first + jnp.arange(row_count, dtype=jnp.int32)
    key_seg = lax.dynamic_slice_in_dim(seg_ids, key_first, row_count, 1)
    needed = (key_first <= query_pos[-1]) & jnp.any(key_seg[:, -1] >= query_seg[:, 0])
    shaped = block.reshape(2, block.shape[1], row_count, query_heads.shape[2], query_heads.shape[3])
    return lax.cond(
        needed,
        lambda state: update(
            state, query_heads, shaped, query_pos, query_seg, key_pos, key_seg, score_scale
        ),
        lambda state: state,
        running,
    )


def body(queries, keys, values, seg_ids, norm_gain, router_w, expert_ids, w_in, w_out):
    my_index = lax.axis_index("seq")
    seq_count, local_len, local_width = queries.shape
    head_count = local_width // HD
    score_scale = HD ** (-0.5)
    first_pos = my_index * local_len
    query_pos = first_pos + jnp.arange(local_len, dtype=jnp.int32)
    query_seg = lax.dynamic_slice_in_dim(seg_ids, first_pos, local_len, 1)
    query_heads = queries.reshape(seq_count, local_len, head_count, HD)
    initial = (
        jnp.full((seq_count, head_count, local_len), NEG, jnp.float32),
        jnp.zeros((seq_count, head_count, local_len), jnp.float32),
        jnp.zeros((seq_count, head_count, local_len, HD), jnp.float32),
    )
    stacked = jnp.stack([keys, values])

    def attend(running, block, key_first):
        return attend_block(
            running, query_heads, block, query_pos, query_seg, seg_ids, key_first, score_scale
        )

    shard_part = lax.all_gather(stacked, "seq", axis=2, tiled=True)
    row_count = shard_part.shape[2]
    width = min(row_count, local_len)
    repeats = row_count // width

    def inner(number, state):
        section = lax.dynamic_slice_in_dim(shard_part, number * width, width, 2)
        return attend(state, section, number * width)

    running = lax.fori_loop(0, repeats, inner, initial)
    maxima, totals, running_total = running
    attended = (
        (running_total / totals[..., None])
        .transpose(0, 2, 1, 3)
        .reshape(seq_count, local_len, local_width)
        .astype(jnp.bfloat16)
    )
    tokens = lax.all_to_all(attended, "exp", split_axis=1, concat_axis=2, tiled=True)
    values32 = tokens.astype(jnp.float32)
    spread = jnp.sqrt(jnp.mean(values32 * values32, axis=-1, keepdims=True) + 1e-06)
    normed = (values32 / spread * norm_gain).astype(jnp.bfloat16)
    token_count = normed.shape[1]
    feature_count = normed.shape[2]
    sub_count = feature_count // SUB
    sub_rows = (
        normed.reshape(seq_count, token_count, sub_count, SUB)
        .transpose(1, 0, 2, 3)
        .reshape(-1, SUB)
    )
    picks = expert_ids.reshape(-1, TOPK)
    logits = jnp.dot(sub_rows, router_w, preferred_element_type=jnp.float32)
    chosen = jnp.take_along_axis(logits, picks, axis=1)
    sigmas = jax.nn.sigmoid(chosen)
    gates = sigmas / jnp.sum(sigmas, axis=1, keepdims=True)
    expert_total = router_w.shape[1]
    targets = picks.reshape(-1)
    one_hot = (targets[:, None] == jnp.arange(expert_total, dtype=jnp.int32)[None, :]).astype(
        jnp.int32
    )
    earlier = jnp.cumsum(one_hot, axis=0) - one_hot
    slot_rank = jnp.sum(earlier * one_hot, axis=1)
    destination = targets * CAP + slot_rank
    sources = jnp.arange(targets.shape[0], dtype=jnp.int32) // TOPK
    outgoing = (
        jnp.zeros((expert_total * CAP, SUB), jnp.bfloat16)
        .at[destination]
        .set(sub_rows[sources])
        .reshape(expert_total, CAP, SUB)
    )
    arrived = lax.all_to_all(outgoing, "exp", split_axis=0, concat_axis=1, tiled=True)
    hidden = jax.nn.gelu(
        jnp.einsum("ecs,esf->ecf", arrived, w_in, preferred_element_type=jnp.float32),
        approximate=True,
    ).astype(jnp.bfloat16)
    results = jnp.einsum("ecf,efs->ecs", hidden, w_out, preferred_element_type=jnp.float32).astype(
        jnp.bfloat16
    )
    returned = lax.all_to_all(results, "exp", split_axis=1, concat_axis=0, tiled=True).reshape(
        expert_total * CAP, SUB
    )
    picked = returned[destination].reshape(-1, TOPK, SUB).astype(jnp.float32)
    mixed = jnp.sum(gates[:, :, None] * picked, axis=1).astype(jnp.bfloat16)
    expert_mix = mixed.reshape(token_count, seq_count, feature_count).transpose(1, 0, 2)
    return (normed, expert_mix)


MESH = pl.DeviceIdType.MESH


LAG = 3
RELAY_BOTH = False


def fused_kernel(
    n_seq, n_exp, per,
    q_ref, k_ref, v_ref, seg_hbm, gain_hbm, router_hbm, ids_hbm, w_in_ref, w_out_ref,
    normed_ref, mix_ref,
    seg_ref, gain_ref, router_ref,
    stage, qkv, probs, inverse, att, rows, idsbuf, norm, partial, own_sum, part_out, part_in, relay_in,
    win, wout,
    w_sem, stage_sem, loc_sem, ids_send, ids_recv, qkv_send, qkv_recv, att_send, att_recv,
    ag_send, ag_recv, rs_send, rs_recv, hop_recv,
):
    seqs, local_len, hd = q_ref.shape
    seq_len = n_seq * local_len
    s = lax.axis_index("seq")
    z = lax.axis_index("exp")
    experts_here = w_in_ref.shape[0]
    tok = local_len // n_exp
    width = rows.shape[2]
    groups = seqs // per
    last = n_exp - 1
    is_end = (z == 0) | (z == last)
    is_mid = (z == 1) | (z == last - 1)
    far = last - z
    near = jnp.where(z <= 1, jnp.where(z == 0, 1, 0), jnp.where(z == last, last - 1, last))
    away = last - near
    inner = last - z

    def arrived(ref, sem):
        return pltpu.make_async_remote_copy(
            src_ref=ref, dst_ref=ref, send_sem=sem, recv_sem=sem,
            device_id={"seq": s, "exp": lax.rem(z + 1, n_exp)}, device_id_type=MESH,
        )

    own_pos = pl.ds(s * local_len, local_len)
    barrier = pltpu.get_barrier_semaphore()
    for d in range(1, n_exp):
        pl.semaphore_signal(
            barrier, inc=1, device_id={"seq": s, "exp": lax.rem(z + d, n_exp)}, device_id_type=MESH
        )
    for d in range(1, n_seq):
        pl.semaphore_signal(
            barrier, inc=1, device_id={"seq": lax.rem(s + d, n_seq), "exp": z}, device_id_type=MESH
        )
    sources = (q_ref, k_ref, v_ref)
    staged = [
        pltpu.make_async_copy(ref, stage.at[i], stage_sem) for i, ref in enumerate(sources)
    ]
    small = [
        pltpu.make_async_copy(seg_hbm, seg_ref, loc_sem.at[0]),
        pltpu.make_async_copy(gain_hbm, gain_ref, loc_sem.at[1]),
        pltpu.make_async_copy(router_hbm, router_ref, loc_sem.at[2]),
    ]
    locals_ = [
        pltpu.make_async_copy(ref.at[s], qkv.at[i, own_pos], qkv_recv.at[i // 2])
        for i, ref in enumerate(sources)
    ]
    own_ids = pltpu.make_async_copy(ids_hbm, idsbuf.at[z], ids_recv)
    w_copies = [
        pltpu.make_async_copy(w_in_ref, win, w_sem.at[0]),
        pltpu.make_async_copy(w_out_ref, wout, w_sem.at[1]),
    ]
    for c in staged + small + locals_ + [own_ids]:
        c.start()
    arrived(stage, stage_sem).wait_recv()
    pl.semaphore_wait(barrier, n_seq + n_exp - 2)

    for i in range(3):
        for d in range(1, n_seq):
            to = lax.rem(s + d, n_seq)
            pltpu.make_async_remote_copy(
                src_ref=stage.at[i, to],
                dst_ref=qkv.at[i, own_pos],
                send_sem=qkv_send,
                recv_sem=qkv_recv.at[i // 2],
                device_id={"seq": to, "exp": z},
                device_id_type=MESH,
            ).start()
    for d in range(1, n_exp):
        pltpu.make_async_remote_copy(
            src_ref=ids_hbm,
            dst_ref=idsbuf.at[z],
            send_sem=ids_send,
            recv_sem=ids_recv,
            device_id={"seq": s, "exp": lax.rem(z + d, n_exp)},
            device_id_type=MESH,
        ).start()
    for c in w_copies:
        c.start()

    for c in small:
        c.wait()
    seg_row = seg_ref[pl.ds(s, 1), :].astype(jnp.float32)
    seg_cols = jnp.broadcast_to(seg_row, (hd, seq_len)).T

    arrived(idsbuf, ids_recv).wait_recv()
    count = per * local_len
    for t in range(TOPK):
        line = jnp.concatenate(
            [idsbuf[e, b, t:t + 1, :] for b in range(seqs) for e in range(n_exp)], axis=1
        ).astype(jnp.float32)
        cols = jnp.broadcast_to(line, (128, line.shape[1])).T
        for g in range(groups):
            partial[t, g] = cols[g * count:(g + 1) * count]

    arrived(qkv.at[pl.ds(0, 2)], qkv_recv.at[0]).wait_recv()
    step = 128
    scale = hd ** (-0.5) * 1.4426950408889634
    for first in range(0, seq_len, step):
        reach = first + step
        scores = lax.dot_general(
            qkv[0, first:reach], qkv[1, :reach], (((1,), (1,)), ((), ())),
            preferred_element_type=jnp.float32,
        )
        qpos = first + lax.broadcasted_iota(jnp.int32, (step, reach), 0)
        kpos = lax.broadcasted_iota(jnp.int32, (step, reach), 1)
        same = jnp.concatenate(
            [seg_cols[first:reach] == seg_row[:, j:j + step] for j in range(0, reach, step)], axis=1
        )
        scores = jnp.where((kpos <= qpos) & same, scores, NEG)
        top = jnp.max(scores, axis=-1, keepdims=True)
        p = jnp.exp2((scores - top) * scale)
        total = jnp.sum(p, axis=-1, keepdims=True)
        probs[first:reach, :reach] = p.astype(jnp.bfloat16)
        inverse[first:reach, :] = jnp.broadcast_to(1.0 / total, (step, hd))
    arrived(qkv.at[2], qkv_recv.at[1]).wait_recv()
    for first in range(0, seq_len, step):
        reach = first + step
        o = jnp.dot(
            probs[first:reach, :reach], qkv[2, :reach], preferred_element_type=jnp.float32
        )
        att[first:reach] = (o * inverse[first:reach]).astype(jnp.bfloat16)

    head = pl.ds(pl.multiple_of(z * hd, hd), hd)
    first_group = s // per
    pltpu.make_async_copy(att.at[own_pos], rows.at[s, :, head], att_recv.at[first_group]).start()
    for d in range(1, n_seq):
        to = lax.rem(s + d, n_seq)
        pltpu.make_async_remote_copy(
            src_ref=att.at[pl.ds(to * local_len, local_len)],
            dst_ref=rows.at[s, :, head],
            send_sem=att_send,
            recv_sem=att_recv.at[first_group],
            device_id={"seq": to, "exp": z},
            device_id_type=MESH,
        ).start()

    def ag_copy(g, owner, to):
        cols = pl.ds(pl.multiple_of(owner * hd, hd), hd)
        there = rows.at[pl.ds(g * per, per), :, cols]
        return pltpu.make_async_remote_copy(
            src_ref=there, dst_ref=there, send_sem=ag_send, recv_sem=ag_recv.at[g],
            device_id={"seq": s, "exp": to}, device_id_type=MESH,
        )

    for i in range(groups):
        g = lax.rem(first_group + i, groups)
        arrived(rows.at[pl.ds(g * per, per), :, head], att_recv.at[g]).wait_recv()
        for d in range(1, n_exp):
            e = lax.rem(z + d, n_exp)
            held = is_end & (e == far)
            if RELAY_BOTH:
                held = held | (is_mid & (e == away))

            @pl.when(~held)
            def _():
                ag_copy(g, z, e).start()

    for c in w_copies:
        c.wait()

    def rs_copy(g, d):
        e = lax.rem(z + d, n_exp)
        return pltpu.make_async_remote_copy(
            src_ref=part_out.at[pl.ds(g * per, per), pl.ds(pl.multiple_of(e * tok, tok), tok), :],
            dst_ref=part_in.at[d, pl.ds(g * per, per)],
            send_sem=rs_send,
            recv_sem=rs_recv.at[g],
            device_id={"seq": s, "exp": e},
            device_id_type=MESH,
        )

    def rs_hop(g):
        place = jnp.where(is_end, far, away)
        part = pl.ds(pl.multiple_of(place * tok, tok), tok)
        return pltpu.make_async_remote_copy(
            src_ref=part_out.at[pl.ds(g * per, per), part, :],
            dst_ref=relay_in.at[pl.ds(g * per, per)],
            send_sem=rs_send,
            recv_sem=hop_recv.at[g],
            device_id={"seq": s, "exp": near},
            device_id_type=MESH,
        )

    mine = pl.ds(pl.multiple_of(z * tok, tok), tok)

    def pass_on(before):
        earlier = pl.ds(before * per, per)
        rs_hop(before).wait_recv()
        part = pl.ds(pl.multiple_of(away * tok, tok), tok)
        both = own_sum[earlier, part, :] + relay_in[earlier].astype(jnp.float32)
        part_out[earlier, part, :] = both.astype(jnp.bfloat16)
        rs_copy(before, lax.rem(away + n_exp - z, n_exp)).start()

    @pl.loop(0, groups)
    def _(i):
        g = lax.rem(first_group + i, groups)
        members = pl.ds(g * per, per)
        arrived(rows.at[members, :, pl.ds(0, width - hd)], ag_recv.at[g]).wait_recv()

        @pl.when(is_mid)
        def _():
            if RELAY_BOTH:
                ag_copy(g, inner, near).start()
            ag_copy(g, away, near).start()

        x = rows[members].reshape(count, width).astype(jnp.float32)
        inv = 1.0 / jnp.sqrt(jnp.mean(x * x, axis=-1, keepdims=True) + 1e-06)
        flat = (x * inv * gain_ref[...]).astype(jnp.bfloat16)
        norm[members] = flat.reshape(per, local_len, width)
        logits = lax.dot_general(
            flat, router_ref[...], (((1,), (1,)), ((), ())), preferred_element_type=jnp.float32
        )
        total = logits.shape[1]
        names = lax.broadcasted_iota(jnp.int32, logits.shape, 1).astype(jnp.float32)
        id0, id1 = partial[0, g], partial[1, g]
        c0 = jnp.sum(jnp.where(names == id0[:, :total], logits, 0.0), axis=-1, keepdims=True)
        c1 = jnp.sum(jnp.where(names == id1[:, :total], logits, 0.0), axis=-1, keepdims=True)
        s0 = 1.0 / (1.0 + jnp.exp(-c0))
        s1 = 1.0 / (1.0 + jnp.exp(-c1))
        half = 0.5 / (s0 + s1)
        g0 = s0 * half
        g1 = s1 * half
        acc = None
        for j in range(experts_here):
            name = (z * experts_here + j).astype(jnp.float32)
            gate = jnp.where(id0 == name, g0, 0.0) + jnp.where(id1 == name, g1, 0.0)
            u = jnp.dot(flat, win[j], preferred_element_type=jnp.float32)
            bent = jnp.tanh(u * (0.7978845608028654 + 0.035677408136300125 * (u * u)))
            scaled = u * jnp.concatenate([gate] * (u.shape[1] // gate.shape[1]), axis=1)
            t = jnp.dot(
                (scaled + scaled * bent).astype(jnp.bfloat16), wout[j],
                preferred_element_type=jnp.float32,
            )
            acc = t if acc is None else acc + t
        acc = acc.reshape(per, local_len, width)
        part_out[members] = acc.astype(jnp.bfloat16)
        own_sum[members] = acc
        direct = i >= groups - LAG

        @pl.when(is_mid & (i >= LAG))
        def _():
            pass_on(lax.rem(first_group + i + groups - LAG, groups))

        for d in range(1, n_exp):
            e = lax.rem(z + d, n_exp)
            held = ~direct & ((is_end & (e == far)) | (is_mid & (e == away)))

            @pl.when(~held)
            def _():
                rs_copy(g, d).start()

        @pl.when(is_end & ~direct)
        def _():
            rs_hop(g).start()

    normed_ref[...] = norm[:, mine, :]
    for i in range(groups):
        g = lax.rem(first_group + i, groups)
        members = pl.ds(g * per, per)
        acc = own_sum[members, mine, :]
        if i >= groups - LAG:
            arrived(part_in.at[pl.ds(0, n_exp - 1), members], rs_recv.at[g]).wait_recv()
        else:
            @pl.when(is_end)
            def _():
                lost = lax.rem(z + n_exp - far, n_exp)
                arrived(part_in.at[pl.ds(0, n_exp - 2), members], rs_recv.at[g]).wait_recv()
                part_in[lost, members] = jnp.zeros((per, tok, width), jnp.bfloat16)

            @pl.when(~is_end)
            def _():
                arrived(part_in.at[pl.ds(0, n_exp - 1), members], rs_recv.at[g]).wait_recv()

        for d in range(1, n_exp):
            acc = acc + part_in[d, members].astype(jnp.float32)
        mix_ref[members] = acc.astype(jnp.bfloat16)

    def sent(ref, sem):
        arrived(ref, sem).wait_send()

    sent(qkv.at[:, pl.ds(0, seq_len - local_len)], qkv_send)
    sent(att.at[pl.ds(0, seq_len - local_len)], att_send)
    sent(idsbuf.at[pl.ds(0, n_exp - 1)], ids_send)
    sent(part_out.at[:, pl.ds(0, local_len - tok), :], rs_send)

    @pl.when(is_mid)
    def _():
        sent(rows, ag_send)

    @pl.when(~is_mid)
    def _():
        sent(rows.at[:, :, pl.ds(0, (n_exp - 2) * hd)], ag_send)


def move_kernel(a_ref, b_ref, to_a, to_b, sems):
    first = pltpu.make_async_copy(a_ref, to_a, sems.at[0])
    second = pltpu.make_async_copy(b_ref, to_b, sems.at[1])
    first.start()
    second.start()
    first.wait()
    second.wait()


def fused_body(n_seq, n_exp, queries, keys, values, seg_ids, norm_gain, router_w, expert_ids, w_in, w_out):
    seqs, local_len, hd = queries.shape
    tok = local_len // n_exp
    per = max(1, 128 // local_len)
    groups = seqs // per
    width = norm_gain.shape[0]
    experts_here, sub, ff = w_in.shape
    seq_len = n_seq * local_len
    ids = expert_ids.reshape(tok, seqs, TOPK).transpose(1, 2, 0)
    bf, f32 = jnp.bfloat16, jnp.float32
    hbm = pl.BlockSpec(memory_space=pltpu.HBM)
    vmem = pl.BlockSpec(memory_space=pltpu.VMEM)
    dma = pltpu.SemaphoreType.DMA
    out = pltpu.VMEM((seqs, tok, width), bf)
    normed, mix = pl.pallas_call(
        functools.partial(fused_kernel, n_seq, n_exp, per),
        out_shape=(out, out),
        in_specs=[hbm] * 9,
        out_specs=(vmem, vmem),
        scratch_shapes=[
            pltpu.VMEM(seg_ids.shape, jnp.int32),
            pltpu.VMEM((1, width), f32),
            pltpu.VMEM(router_w.shape[::-1], bf),
            pltpu.VMEM((3, seqs, local_len, hd), bf),
            pltpu.VMEM((3, seq_len, hd), bf),
            pltpu.VMEM((seq_len, seq_len), bf),
            pltpu.VMEM((seq_len, hd), f32),
            pltpu.VMEM((seq_len, hd), bf),
            pltpu.VMEM((seqs, local_len, width), bf),
            pltpu.VMEM((n_exp, seqs, TOPK, tok), jnp.int32),
            pltpu.VMEM((seqs, local_len, width), bf),
            pltpu.VMEM((TOPK, groups, per * local_len, 128), f32),
            pltpu.VMEM((seqs, local_len, width), f32),
            pltpu.VMEM((seqs, local_len, width), bf),
            pltpu.VMEM((n_exp, seqs, tok, width), bf),
            pltpu.VMEM((seqs, tok, width), bf),
            pltpu.VMEM((experts_here, sub, ff), bf),
            pltpu.VMEM((experts_here, ff, sub), bf),
            dma((2,)), dma(()), dma((3,)), dma(()), dma(()), dma(()), dma((2,)), dma(()), dma((groups,)),
            dma(()), dma((groups,)), dma(()), dma((groups,)), dma((groups,)),
        ],
        compiler_params=pltpu.CompilerParams(
            collective_id=0, has_side_effects=True, vmem_limit_bytes=60 * 1024 * 1024
        ),
    )(queries, keys, values, seg_ids, norm_gain.reshape(1, width), router_w.T, ids, w_in, w_out)
    result = jax.ShapeDtypeStruct((seqs, tok, width), bf)
    return pl.pallas_call(
        move_kernel,
        out_shape=(result, result),
        in_specs=[pl.BlockSpec(memory_space=pl.ANY)] * 2,
        out_specs=(hbm, hbm),
        scratch_shapes=[dma((2,))],
        compiler_params=pltpu.CompilerParams(vmem_limit_bytes=1024 * 1024),
    )(normed, mix)


def whole_body(n_seq, n_exp, *args):
    queries, norm_gain = args[0], args[4]
    seqs, local_len, width = queries.shape
    fits = (
        seqs == n_seq and width == HD and norm_gain.shape[0] == SUB
        and local_len % (16 * n_exp) == 0 and (local_len * n_seq) % 128 == 0
        and seqs % max(1, 128 // local_len) == 0 and n_exp == 4
    )
    return fused_body(n_seq, n_exp, *args) if fits else body(*args)


def solution(mesh):
    return jax.shard_map(
        functools.partial(whole_body, mesh.shape["seq"], mesh.shape["exp"]),
        mesh=mesh,
        in_specs=(
            P(None, "seq", "exp"),
            P(None, "seq", "exp"),
            P(None, "seq", "exp"),
            P(),
            P(),
            P(),
            P(("seq", "exp"), None, None, None),
            P("exp", None, None),
            P("exp", None, None),
        ),
        out_specs=(P(None, ("seq", "exp"), None), P(None, ("seq", "exp"), None)),
        check_vma=False,
    )
```

```python
import functools

import jax
import jax.numpy as jnp
from jax import lax
from jax.experimental import pallas as pl
from jax.experimental.pallas import tpu as pltpu
from jax.sharding import PartitionSpec as P

HD = 128
SUB = 512
TOPK = 2
CAP = 32


NEG = -1e30


def update(running, query_heads, shaped, query_pos, query_seg, key_pos, key_seg, score_scale):
    maxima, totals, running_total = running
    attention_scores = (
        jnp.einsum("bqhd,bkhd->bhqk", query_heads, shaped[0], preferred_element_type=jnp.float32)
        * score_scale
    )
    visible = (key_pos[None, :] <= query_pos[:, None])[None, None] & (
        key_seg[:, None, None, :] == query_seg[:, None, :, None]
    )
    highest = jnp.max(jnp.where(visible, attention_scores, NEG), axis=-1)
    new_max = jnp.maximum(maxima, highest)
    weights = jnp.where(visible, jnp.exp(attention_scores - new_max[..., None]), 0.0)
    rescale_factor = jnp.exp(maxima - new_max)
    totals = totals * rescale_factor + jnp.sum(weights, axis=-1)
    rounded_result = weights.astype(jnp.bfloat16)
    running_total = running_total * rescale_factor[..., None] + jnp.einsum(
        "bhqk,bkhd->bhqd", rounded_result, shaped[1], preferred_element_type=jnp.float32
    )
    return (new_max, totals, running_total)


def attend_block(
    running, query_heads, block, query_pos, query_seg, seg_ids, key_first, score_scale
):
    row_count = block.shape[2]
    key_pos = key_first + jnp.arange(row_count, dtype=jnp.int32)
    key_seg = lax.dynamic_slice_in_dim(seg_ids, key_first, row_count, 1)
    needed = (key_first <= query_pos[-1]) & jnp.any(key_seg[:, -1] >= query_seg[:, 0])
    shaped = block.reshape(2, block.shape[1], row_count, query_heads.shape[2], query_heads.shape[3])
    return lax.cond(
        needed,
        lambda state: update(
            state, query_heads, shaped, query_pos, query_seg, key_pos, key_seg, score_scale
        ),
        lambda state: state,
        running,
    )


def body(queries, keys, values, seg_ids, norm_gain, router_w, expert_ids, w_in, w_out):
    my_index = lax.axis_index("seq")
    seq_count, local_len, local_width = queries.shape
    head_count = local_width // HD
    score_scale = HD ** (-0.5)
    first_pos = my_index * local_len
    query_pos = first_pos + jnp.arange(local_len, dtype=jnp.int32)
    query_seg = lax.dynamic_slice_in_dim(seg_ids, first_pos, local_len, 1)
    query_heads = queries.reshape(seq_count, local_len, head_count, HD)
    initial = (
        jnp.full((seq_count, head_count, local_len), NEG, jnp.float32),
        jnp.zeros((seq_count, head_count, local_len), jnp.float32),
        jnp.zeros((seq_count, head_count, local_len, HD), jnp.float32),
    )
    stacked = jnp.stack([keys, values])

    def attend(running, block, key_first):
        return attend_block(
            running, query_heads, block, query_pos, query_seg, seg_ids, key_first, score_scale
        )

    shard_part = lax.all_gather(stacked, "seq", axis=2, tiled=True)
    row_count = shard_part.shape[2]
    width = min(row_count, local_len)
    repeats = row_count // width

    def inner(number, state):
        section = lax.dynamic_slice_in_dim(shard_part, number * width, width, 2)
        return attend(state, section, number * width)

    running = lax.fori_loop(0, repeats, inner, initial)
    maxima, totals, running_total = running
    attended = (
        (running_total / totals[..., None])
        .transpose(0, 2, 1, 3)
        .reshape(seq_count, local_len, local_width)
        .astype(jnp.bfloat16)
    )
    tokens = lax.all_to_all(attended, "exp", split_axis=1, concat_axis=2, tiled=True)
    values32 = tokens.astype(jnp.float32)
    spread = jnp.sqrt(jnp.mean(values32 * values32, axis=-1, keepdims=True) + 1e-06)
    normed = (values32 / spread * norm_gain).astype(jnp.bfloat16)
    token_count = normed.shape[1]
    feature_count = normed.shape[2]
    sub_count = feature_count // SUB
    sub_rows = (
        normed.reshape(seq_count, token_count, sub_count, SUB)
        .transpose(1, 0, 2, 3)
        .reshape(-1, SUB)
    )
    picks = expert_ids.reshape(-1, TOPK)
    logits = jnp.dot(sub_rows, router_w, preferred_element_type=jnp.float32)
    chosen = jnp.take_along_axis(logits, picks, axis=1)
    sigmas = jax.nn.sigmoid(chosen)
    gates = sigmas / jnp.sum(sigmas, axis=1, keepdims=True)
    expert_total = router_w.shape[1]
    targets = picks.reshape(-1)
    one_hot = (targets[:, None] == jnp.arange(expert_total, dtype=jnp.int32)[None, :]).astype(
        jnp.int32
    )
    earlier = jnp.cumsum(one_hot, axis=0) - one_hot
    slot_rank = jnp.sum(earlier * one_hot, axis=1)
    destination = targets * CAP + slot_rank
    sources = jnp.arange(targets.shape[0], dtype=jnp.int32) // TOPK
    outgoing = (
        jnp.zeros((expert_total * CAP, SUB), jnp.bfloat16)
        .at[destination]
        .set(sub_rows[sources])
        .reshape(expert_total, CAP, SUB)
    )
    arrived = lax.all_to_all(outgoing, "exp", split_axis=0, concat_axis=1, tiled=True)
    hidden = jax.nn.gelu(
        jnp.einsum("ecs,esf->ecf", arrived, w_in, preferred_element_type=jnp.float32),
        approximate=True,
    ).astype(jnp.bfloat16)
    results = jnp.einsum("ecf,efs->ecs", hidden, w_out, preferred_element_type=jnp.float32).astype(
        jnp.bfloat16
    )
    returned = lax.all_to_all(results, "exp", split_axis=1, concat_axis=0, tiled=True).reshape(
        expert_total * CAP, SUB
    )
    picked = returned[destination].reshape(-1, TOPK, SUB).astype(jnp.float32)
    mixed = jnp.sum(gates[:, :, None] * picked, axis=1).astype(jnp.bfloat16)
    expert_mix = mixed.reshape(token_count, seq_count, feature_count).transpose(1, 0, 2)
    return (normed, expert_mix)


MESH = pl.DeviceIdType.MESH


RELAYED = 2
CHUNK = 256
AHEAD = 1


def fused_kernel(
    n_seq, n_exp, per,
    q_ref, k_ref, v_ref, seg_hbm, gain_hbm, router_hbm, ids_hbm, w_in_ref, w_out_ref,
    normed_ref, mix_ref,
    seg_ref, gain_ref, router_ref,
    stage, qkv, probs, inverse, att, rows, idsbuf, partial, own_sum, part_out, part_in, relay_in,
    hidden, win, wout,
    w_sem, stage_sem, loc_sem, ids_send, ids_recv, qkv_send, qkv_recv, att_send, att_recv,
    ag_send, far_send, ag_recv, rs_send, rs_recv, hop_recv,
):
    seqs, local_len, hd = q_ref.shape
    seq_len = n_seq * local_len
    s = lax.axis_index("seq")
    z = lax.axis_index("exp")
    experts_here = w_in_ref.shape[0]
    tok = local_len // n_exp
    width = rows.shape[2]
    groups = seqs // per
    last = n_exp - 1
    is_end = (z == 0) | (z == last)
    is_mid = (z == 1) | (z == last - 1)
    far = last - z
    near = jnp.where(z <= 1, jnp.where(z == 0, 1, 0), jnp.where(z == last, last - 1, last))
    away = last - near

    def arrived(ref, sem):
        return pltpu.make_async_remote_copy(
            src_ref=ref, dst_ref=ref, send_sem=sem, recv_sem=sem,
            device_id={"seq": s, "exp": lax.rem(z + 1, n_exp)}, device_id_type=MESH,
        )

    chip = s // 2
    if n_seq == 8:
        chips = (3 - chip, lax.rem(chip + 2, 4), chip + 1 - 2 * lax.rem(chip, 2))
        peers = [2 * c + k for c in chips for k in range(2)] + [s + 1 - 2 * lax.rem(s, 2)]
    else:
        peers = [lax.rem(s + d, n_seq) for d in range(1, n_seq)]

    own_pos = pl.ds(s * local_len, local_len)
    barrier = pltpu.get_barrier_semaphore()
    for d in range(1, n_exp):
        pl.semaphore_signal(
            barrier, inc=1, device_id={"seq": s, "exp": lax.rem(z + d, n_exp)}, device_id_type=MESH
        )
    for d in range(1, n_seq):
        pl.semaphore_signal(
            barrier, inc=1, device_id={"seq": lax.rem(s + d, n_seq), "exp": z}, device_id_type=MESH
        )
    sources = (q_ref, k_ref, v_ref)
    staged = [
        pltpu.make_async_copy(ref, stage.at[i], stage_sem) for i, ref in enumerate(sources)
    ]
    small = [
        pltpu.make_async_copy(seg_hbm, seg_ref, loc_sem.at[0]),
        pltpu.make_async_copy(gain_hbm, gain_ref, loc_sem.at[1]),
        pltpu.make_async_copy(router_hbm, router_ref, loc_sem.at[2]),
    ]
    locals_ = [
        pltpu.make_async_copy(ref.at[s], qkv.at[i, own_pos], qkv_recv.at[i // 2])
        for i, ref in enumerate(sources)
    ]
    own_ids = pltpu.make_async_copy(ids_hbm, idsbuf.at[z], ids_recv)
    w_copies = [
        pltpu.make_async_copy(w_in_ref, win, w_sem.at[0]),
        pltpu.make_async_copy(w_out_ref, wout, w_sem.at[1]),
    ]
    for c in staged + small + locals_ + [own_ids]:
        c.start()
    arrived(stage, stage_sem).wait_recv()
    pl.semaphore_wait(barrier, n_seq + n_exp - 2)

    for i in range(3):
        for to in peers:
            pltpu.make_async_remote_copy(
                src_ref=stage.at[i, to],
                dst_ref=qkv.at[i, own_pos],
                send_sem=qkv_send,
                recv_sem=qkv_recv.at[i // 2],
                device_id={"seq": to, "exp": z},
                device_id_type=MESH,
            ).start()
    for d in range(1, n_exp):
        pltpu.make_async_remote_copy(
            src_ref=ids_hbm,
            dst_ref=idsbuf.at[z],
            send_sem=ids_send,
            recv_sem=ids_recv,
            device_id={"seq": s, "exp": lax.rem(z + d, n_exp)},
            device_id_type=MESH,
        ).start()
    for c in w_copies:
        c.start()

    for c in small:
        c.wait()
    seg_row = seg_ref[pl.ds(s, 1), :].astype(jnp.float32)
    seg_cols = jnp.broadcast_to(seg_row, (hd, seq_len)).T

    arrived(idsbuf, ids_recv).wait_recv()
    count = per * local_len
    for t in range(TOPK):
        line = jnp.concatenate(
            [idsbuf[e, b, t:t + 1, :] for b in range(seqs) for e in range(n_exp)], axis=1
        ).astype(jnp.float32)
        cols = jnp.broadcast_to(line, (128, line.shape[1])).T
        for g in range(groups):
            partial[t, g] = cols[g * count:(g + 1) * count]

    arrived(qkv.at[pl.ds(0, 2)], qkv_recv.at[0]).wait_recv()
    step = 128
    scale = hd ** (-0.5) * 1.4426950408889634
    for first in range(0, seq_len, step):
        reach = first + step
        scores = lax.dot_general(
            qkv[0, first:reach], qkv[1, :reach], (((1,), (1,)), ((), ())),
            preferred_element_type=jnp.float32,
        )
        qpos = first + lax.broadcasted_iota(jnp.int32, (step, reach), 0)
        kpos = lax.broadcasted_iota(jnp.int32, (step, reach), 1)
        same = jnp.concatenate(
            [seg_cols[first:reach] == seg_row[:, j:j + step] for j in range(0, reach, step)], axis=1
        )
        scores = jnp.where((kpos <= qpos) & same, scores, NEG)
        top = jnp.max(scores, axis=-1, keepdims=True)
        p = jnp.exp2((scores - top) * scale)
        total = jnp.sum(p, axis=-1, keepdims=True)
        probs[first:reach, :reach] = p.astype(jnp.bfloat16)
        inverse[first:reach, :] = jnp.broadcast_to(1.0 / total, (step, hd))
    arrived(qkv.at[2], qkv_recv.at[1]).wait_recv()
    for first in range(0, seq_len, step):
        reach = first + step
        o = jnp.dot(
            probs[first:reach, :reach], qkv[2, :reach], preferred_element_type=jnp.float32
        )
        att[first:reach] = (o * inverse[first:reach]).astype(jnp.bfloat16)

    head = pl.ds(pl.multiple_of(z * hd, hd), hd)
    first_group = s // per
    pltpu.make_async_copy(att.at[own_pos], rows.at[s, :, head], att_recv.at[first_group]).start()
    for to in peers[-1:] + peers[:-1]:
        pltpu.make_async_remote_copy(
            src_ref=att.at[pl.ds(to * local_len, local_len)],
            dst_ref=rows.at[s, :, head],
            send_sem=att_send,
            recv_sem=att_recv.at[first_group],
            device_id={"seq": to, "exp": z},
            device_id_type=MESH,
        ).start()

    def ag_copy(g, owner, to, sem):
        cols = pl.ds(pl.multiple_of(owner * hd, hd), hd)
        there = rows.at[pl.ds(g * per, per), :, cols]
        return pltpu.make_async_remote_copy(
            src_ref=there, dst_ref=there, send_sem=sem, recv_sem=ag_recv.at[g],
            device_id={"seq": s, "exp": to}, device_id_type=MESH,
        )

    for i in range(groups):
        g = lax.rem(first_group + i, groups)
        arrived(rows.at[pl.ds(g * per, per), :, head], att_recv.at[g]).wait_recv()
        for d in range(1, n_exp):
            e = lax.rem(z + d, n_exp)
            @pl.when(~(is_end & (e == far)))
            def _():
                ag_copy(g, z, e, ag_send).start()

    for c in w_copies:
        c.wait()

    def rs_copy(g, d):
        e = lax.rem(z + d, n_exp)
        return pltpu.make_async_remote_copy(
            src_ref=part_out.at[pl.ds(g * per, per), pl.ds(pl.multiple_of(e * tok, tok), tok), :],
            dst_ref=part_in.at[d, pl.ds(g * per, per)],
            send_sem=rs_send,
            recv_sem=rs_recv.at[g],
            device_id={"seq": s, "exp": e},
            device_id_type=MESH,
        )

    def rs_hop(g):
        place = jnp.where(is_end, far, away)
        part = pl.ds(pl.multiple_of(place * tok, tok), tok)
        return pltpu.make_async_remote_copy(
            src_ref=part_out.at[pl.ds(g * per, per), part, :],
            dst_ref=relay_in.at[pl.ds(g * per, per)],
            send_sem=rs_send,
            recv_sem=hop_recv.at[g],
            device_id={"seq": s, "exp": near},
            device_id_type=MESH,
        )

    def pass_on(before):
        earlier = pl.ds(before * per, per)
        rs_hop(before).wait_recv()
        part = pl.ds(pl.multiple_of(away * tok, tok), tok)
        both = own_sum[earlier, part, :] + relay_in[earlier].astype(jnp.float32)
        part_out[earlier, part, :] = both.astype(jnp.bfloat16)
        rs_copy(before, lax.rem(away + n_exp - z, n_exp)).start()

    def gathered(g):
        arrived(rows.at[pl.ds(g * per, per), :, pl.ds(0, width - hd)], ag_recv.at[g]).wait_recv()

    mine = pl.ds(pl.multiple_of(z * tok, tok), tok)

    @pl.loop(0, groups)
    def _(i):
        g = lax.rem(first_group + i, groups)
        members = pl.ds(g * per, per)
        gathered(g)

        @pl.when(is_mid)
        def _():
            ag_copy(g, away, near, far_send).start()

        x = rows[members].reshape(count, width).astype(jnp.float32)
        inv = 1.0 / jnp.sqrt(jnp.mean(x * x, axis=-1, keepdims=True) + 1e-06)
        flat = (x * gain_ref[...]).astype(jnp.bfloat16)
        logits = inv * lax.dot_general(
            flat, router_ref[...], (((1,), (1,)), ((), ())), preferred_element_type=jnp.float32
        )
        total = logits.shape[1]
        names = lax.broadcasted_iota(jnp.int32, logits.shape, 1).astype(jnp.float32)
        id0, id1 = partial[0, g], partial[1, g]
        c0 = jnp.sum(jnp.where(names == id0[:, :total], logits, 0.0), axis=-1, keepdims=True)
        c1 = jnp.sum(jnp.where(names == id1[:, :total], logits, 0.0), axis=-1, keepdims=True)
        s0 = 1.0 / (1.0 + jnp.exp(-c0))
        s1 = 1.0 / (1.0 + jnp.exp(-c1))
        half = 0.5 / (s0 + s1)
        g0 = s0 * half
        g1 = s1 * half
        acc = None
        for j in range(experts_here + AHEAD):
            if j < experts_here:
                name = (z * experts_here + j).astype(jnp.float32)
                gate = jnp.where(id0 == name, g0, 0.0) + jnp.where(id1 == name, g1, 0.0)
                gate = jnp.concatenate([gate * inv] * (CHUNK // gate.shape[1]), axis=1)
                for c in range(0, hidden.shape[2], CHUNK):
                    u = jnp.dot(flat, win[j, :, c:c + CHUNK], preferred_element_type=jnp.float32)
                    scaled = u * gate
                    u = u * inv
                    bent = jnp.tanh(u * (0.7978845608028654 + 0.035677408136300125 * (u * u)))
                    hidden[j, :, c:c + CHUNK] = (scaled + scaled * bent).astype(jnp.bfloat16)
            if j >= AHEAD:
                t = jnp.dot(
                    hidden[j - AHEAD], wout[j - AHEAD], preferred_element_type=jnp.float32
                )
                acc = t if acc is None else acc + t
        acc = acc.reshape(per, local_len, width)
        part_out[members] = acc.astype(jnp.bfloat16)
        own_sum[members] = acc
        direct = i >= RELAYED

        @pl.when(is_end & direct)
        def _():
            rs_copy(g, lax.rem(far + n_exp - z, n_exp)).start()

        for d in range(1, n_exp):
            e = lax.rem(z + d, n_exp)

            @pl.when(is_end & (e != far) & (i == groups - 1))
            def _():
                rs_copy(lax.rem(g + groups - 1, groups), d).start()

        for d in range(1, n_exp):
            e = lax.rem(z + d, n_exp)
            held = (is_end & ((e == far) | (i == groups - 2))) | (is_mid & ~direct & (e == away))

            @pl.when(~held)
            def _():
                rs_copy(g, d).start()

        @pl.when(is_end & ~direct)
        def _():
            rs_hop(g).start()

    @pl.when(is_mid)
    def _():
        for i in range(RELAYED):
            pass_on(lax.rem(first_group + i, groups))

    for i in range(groups):
        g = lax.rem(first_group + i, groups)
        members = pl.ds(g * per, per)
        x = rows[members, mine, :].astype(jnp.float32)
        inv = 1.0 / jnp.sqrt(jnp.mean(x * x, axis=-1, keepdims=True) + 1e-06)
        normed_ref[members] = (x * inv * gain_ref[...]).astype(jnp.bfloat16)
        acc = own_sum[members, mine, :]
        if i >= RELAYED:
            arrived(part_in.at[pl.ds(0, n_exp - 1), members], rs_recv.at[g]).wait_recv()
        else:
            @pl.when(is_end)
            def _():
                lost = lax.rem(z + n_exp - far, n_exp)
                arrived(part_in.at[pl.ds(0, n_exp - 2), members], rs_recv.at[g]).wait_recv()
                part_in[lost, members] = jnp.zeros((per, tok, width), jnp.bfloat16)

            @pl.when(~is_end)
            def _():
                arrived(part_in.at[pl.ds(0, n_exp - 1), members], rs_recv.at[g]).wait_recv()

        for d in range(1, n_exp):
            acc = acc + part_in[d, members].astype(jnp.float32)
        mix_ref[members] = acc.astype(jnp.bfloat16)

    def sent(ref, sem):
        arrived(ref, sem).wait_send()

    sent(qkv.at[:, pl.ds(0, seq_len - local_len)], qkv_send)
    sent(att.at[pl.ds(0, seq_len - local_len)], att_send)
    sent(idsbuf.at[pl.ds(0, n_exp - 1)], ids_send)
    sent(part_out.at[:, pl.ds(0, local_len - tok), :], rs_send)

    @pl.when(is_mid)
    def _():
        sent(rows.at[:, :, pl.ds(0, (n_exp - 1) * hd)], ag_send)
        sent(rows.at[:, :, pl.ds(0, hd)], far_send)

    @pl.when(~is_mid)
    def _():
        sent(rows.at[:, :, pl.ds(0, (n_exp - 2) * hd)], ag_send)


def move_kernel(a_ref, b_ref, to_a, to_b, sems):
    first = pltpu.make_async_copy(a_ref, to_a, sems.at[0])
    second = pltpu.make_async_copy(b_ref, to_b, sems.at[1])
    first.start()
    second.start()
    first.wait()
    second.wait()


def fused_body(n_seq, n_exp, queries, keys, values, seg_ids, norm_gain, router_w, expert_ids, w_in, w_out):
    seqs, local_len, hd = queries.shape
    tok = local_len // n_exp
    per = max(1, 128 // local_len)
    groups = seqs // per
    width = norm_gain.shape[0]
    experts_here, sub, ff = w_in.shape
    seq_len = n_seq * local_len
    ids = expert_ids.reshape(tok, seqs, TOPK).transpose(1, 2, 0)
    bf, f32 = jnp.bfloat16, jnp.float32
    hbm = pl.BlockSpec(memory_space=pltpu.HBM)
    vmem = pl.BlockSpec(memory_space=pltpu.VMEM)
    dma = pltpu.SemaphoreType.DMA
    out = pltpu.VMEM((seqs, tok, width), bf)
    normed, mix = pl.pallas_call(
        functools.partial(fused_kernel, n_seq, n_exp, per),
        out_shape=(out, out),
        in_specs=[hbm] * 9,
        out_specs=(vmem, vmem),
        scratch_shapes=[
            pltpu.VMEM(seg_ids.shape, jnp.int32),
            pltpu.VMEM((1, width), f32),
            pltpu.VMEM(router_w.shape[::-1], bf),
            pltpu.VMEM((3, seqs, local_len, hd), bf),
            pltpu.VMEM((3, seq_len, hd), bf),
            pltpu.VMEM((seq_len, seq_len), bf),
            pltpu.VMEM((seq_len, hd), f32),
            pltpu.VMEM((seq_len, hd), bf),
            pltpu.VMEM((seqs, local_len, width), bf),
            pltpu.VMEM((n_exp, seqs, TOPK, tok), jnp.int32),
            pltpu.VMEM((TOPK, groups, per * local_len, 128), f32),
            pltpu.VMEM((seqs, local_len, width), f32),
            pltpu.VMEM((seqs, local_len, width), bf),
            pltpu.VMEM((n_exp, seqs, tok, width), bf),
            pltpu.VMEM((seqs, tok, width), bf),
            pltpu.VMEM((experts_here, per * local_len, ff), bf),
            pltpu.VMEM((experts_here, sub, ff), bf),
            pltpu.VMEM((experts_here, ff, sub), bf),
            dma((2,)), dma(()), dma((3,)), dma(()), dma(()), dma(()), dma((2,)), dma(()), dma((groups,)),
            dma(()), dma(()), dma((groups,)), dma(()), dma((groups,)), dma((groups,)),
        ],
        compiler_params=pltpu.CompilerParams(
            collective_id=0, has_side_effects=True, vmem_limit_bytes=60 * 1024 * 1024
        ),
    )(queries, keys, values, seg_ids, norm_gain.reshape(1, width), router_w.T, ids, w_in, w_out)
    result = jax.ShapeDtypeStruct((seqs, tok, width), bf)
    return pl.pallas_call(
        move_kernel,
        out_shape=(result, result),
        in_specs=[pl.BlockSpec(memory_space=pl.ANY)] * 2,
        out_specs=(hbm, hbm),
        scratch_shapes=[dma((2,))],
        compiler_params=pltpu.CompilerParams(vmem_limit_bytes=1024 * 1024),
    )(normed, mix)


def whole_body(n_seq, n_exp, *args):
    queries, norm_gain = args[0], args[4]
    seqs, local_len, width = queries.shape
    fits = (
        seqs == n_seq and width == HD and norm_gain.shape[0] == SUB
        and local_len % (16 * n_exp) == 0 and (local_len * n_seq) % 128 == 0
        and seqs % max(1, 128 // local_len) == 0 and n_exp == 4
    )
    return fused_body(n_seq, n_exp, *args) if fits else body(*args)


def solution(mesh):
    return jax.shard_map(
        functools.partial(whole_body, mesh.shape["seq"], mesh.shape["exp"]),
        mesh=mesh,
        in_specs=(
            P(None, "seq", "exp"),
            P(None, "seq", "exp"),
            P(None, "seq", "exp"),
            P(),
            P(),
            P(),
            P(("seq", "exp"), None, None, None),
            P("exp", None, None),
            P("exp", None, None),
        ),
        out_specs=(P(None, ("seq", "exp"), None), P(None, ("seq", "exp"), None)),
        check_vma=False,
    )
```

```python
import functools

import jax
import jax.numpy as jnp
from jax import lax
from jax.experimental import pallas as pl
from jax.experimental.pallas import tpu as pltpu
from jax.sharding import PartitionSpec as P

HD = 128
SUB = 512
TOPK = 2
CAP = 32


NEG = -1e30


def update(running, query_heads, shaped, query_pos, query_seg, key_pos, key_seg, score_scale):
    maxima, totals, running_total = running
    attention_scores = (
        jnp.einsum("bqhd,bkhd->bhqk", query_heads, shaped[0], preferred_element_type=jnp.float32)
        * score_scale
    )
    visible = (key_pos[None, :] <= query_pos[:, None])[None, None] & (
        key_seg[:, None, None, :] == query_seg[:, None, :, None]
    )
    highest = jnp.max(jnp.where(visible, attention_scores, NEG), axis=-1)
    new_max = jnp.maximum(maxima, highest)
    weights = jnp.where(visible, jnp.exp(attention_scores - new_max[..., None]), 0.0)
    rescale_factor = jnp.exp(maxima - new_max)
    totals = totals * rescale_factor + jnp.sum(weights, axis=-1)
    rounded_result = weights.astype(jnp.bfloat16)
    running_total = running_total * rescale_factor[..., None] + jnp.einsum(
        "bhqk,bkhd->bhqd", rounded_result, shaped[1], preferred_element_type=jnp.float32
    )
    return (new_max, totals, running_total)


def attend_block(
    running, query_heads, block, query_pos, query_seg, seg_ids, key_first, score_scale
):
    row_count = block.shape[2]
    key_pos = key_first + jnp.arange(row_count, dtype=jnp.int32)
    key_seg = lax.dynamic_slice_in_dim(seg_ids, key_first, row_count, 1)
    needed = (key_first <= query_pos[-1]) & jnp.any(key_seg[:, -1] >= query_seg[:, 0])
    shaped = block.reshape(2, block.shape[1], row_count, query_heads.shape[2], query_heads.shape[3])
    return lax.cond(
        needed,
        lambda state: update(
            state, query_heads, shaped, query_pos, query_seg, key_pos, key_seg, score_scale
        ),
        lambda state: state,
        running,
    )


def body(queries, keys, values, seg_ids, norm_gain, router_w, expert_ids, w_in, w_out):
    my_index = lax.axis_index("seq")
    seq_count, local_len, local_width = queries.shape
    head_count = local_width // HD
    score_scale = HD ** (-0.5)
    first_pos = my_index * local_len
    query_pos = first_pos + jnp.arange(local_len, dtype=jnp.int32)
    query_seg = lax.dynamic_slice_in_dim(seg_ids, first_pos, local_len, 1)
    query_heads = queries.reshape(seq_count, local_len, head_count, HD)
    initial = (
        jnp.full((seq_count, head_count, local_len), NEG, jnp.float32),
        jnp.zeros((seq_count, head_count, local_len), jnp.float32),
        jnp.zeros((seq_count, head_count, local_len, HD), jnp.float32),
    )
    stacked = jnp.stack([keys, values])

    def attend(running, block, key_first):
        return attend_block(
            running, query_heads, block, query_pos, query_seg, seg_ids, key_first, score_scale
        )

    shard_part = lax.all_gather(stacked, "seq", axis=2, tiled=True)
    row_count = shard_part.shape[2]
    width = min(row_count, local_len)
    repeats = row_count // width

    def inner(number, state):
        section = lax.dynamic_slice_in_dim(shard_part, number * width, width, 2)
        return attend(state, section, number * width)

    running = lax.fori_loop(0, repeats, inner, initial)
    maxima, totals, running_total = running
    attended = (
        (running_total / totals[..., None])
        .transpose(0, 2, 1, 3)
        .reshape(seq_count, local_len, local_width)
        .astype(jnp.bfloat16)
    )
    tokens = lax.all_to_all(attended, "exp", split_axis=1, concat_axis=2, tiled=True)
    values32 = tokens.astype(jnp.float32)
    spread = jnp.sqrt(jnp.mean(values32 * values32, axis=-1, keepdims=True) + 1e-06)
    normed = (values32 / spread * norm_gain).astype(jnp.bfloat16)
    token_count = normed.shape[1]
    feature_count = normed.shape[2]
    sub_count = feature_count // SUB
    sub_rows = (
        normed.reshape(seq_count, token_count, sub_count, SUB)
        .transpose(1, 0, 2, 3)
        .reshape(-1, SUB)
    )
    picks = expert_ids.reshape(-1, TOPK)
    logits = jnp.dot(sub_rows, router_w, preferred_element_type=jnp.float32)
    chosen = jnp.take_along_axis(logits, picks, axis=1)
    sigmas = jax.nn.sigmoid(chosen)
    gates = sigmas / jnp.sum(sigmas, axis=1, keepdims=True)
    expert_total = router_w.shape[1]
    targets = picks.reshape(-1)
    one_hot = (targets[:, None] == jnp.arange(expert_total, dtype=jnp.int32)[None, :]).astype(
        jnp.int32
    )
    earlier = jnp.cumsum(one_hot, axis=0) - one_hot
    slot_rank = jnp.sum(earlier * one_hot, axis=1)
    destination = targets * CAP + slot_rank
    sources = jnp.arange(targets.shape[0], dtype=jnp.int32) // TOPK
    outgoing = (
        jnp.zeros((expert_total * CAP, SUB), jnp.bfloat16)
        .at[destination]
        .set(sub_rows[sources])
        .reshape(expert_total, CAP, SUB)
    )
    arrived = lax.all_to_all(outgoing, "exp", split_axis=0, concat_axis=1, tiled=True)
    hidden = jax.nn.gelu(
        jnp.einsum("ecs,esf->ecf", arrived, w_in, preferred_element_type=jnp.float32),
        approximate=True,
    ).astype(jnp.bfloat16)
    results = jnp.einsum("ecf,efs->ecs", hidden, w_out, preferred_element_type=jnp.float32).astype(
        jnp.bfloat16
    )
    returned = lax.all_to_all(results, "exp", split_axis=1, concat_axis=0, tiled=True).reshape(
        expert_total * CAP, SUB
    )
    picked = returned[destination].reshape(-1, TOPK, SUB).astype(jnp.float32)
    mixed = jnp.sum(gates[:, :, None] * picked, axis=1).astype(jnp.bfloat16)
    expert_mix = mixed.reshape(token_count, seq_count, feature_count).transpose(1, 0, 2)
    return (normed, expert_mix)


MESH = pl.DeviceIdType.MESH


RELAYED = 2
CHUNK = 256
AHEAD = 1


def fused_kernel(
    n_seq, n_exp, per,
    q_ref, k_ref, v_ref, seg_hbm, gain_hbm, router_hbm, ids_hbm, w_in_ref, w_out_ref,
    normed_ref, mix_ref,
    seg_ref, gain_ref, router_ref,
    stage, qkv, probs, inverse, att, rows, idsbuf, partial, own_sum, part_out, part_in, relay_in,
    hidden, win, wout,
    w_sem, stage_sem, loc_sem, ids_send, ids_recv, qkv_send, qkv_recv, att_send, att_recv,
    ag_send, far_send, ag_recv, rs_send, rs_recv, hop_recv,
):
    seqs, local_len, hd = q_ref.shape
    seq_len = n_seq * local_len
    s = lax.axis_index("seq")
    z = lax.axis_index("exp")
    experts_here = w_in_ref.shape[0]
    tok = local_len // n_exp
    width = rows.shape[2]
    groups = seqs // per
    last = n_exp - 1
    is_end = (z == 0) | (z == last)
    is_mid = (z == 1) | (z == last - 1)
    far = last - z
    near = jnp.where(z <= 1, jnp.where(z == 0, 1, 0), jnp.where(z == last, last - 1, last))
    away = last - near

    def arrived(ref, sem):
        return pltpu.make_async_remote_copy(
            src_ref=ref, dst_ref=ref, send_sem=sem, recv_sem=sem,
            device_id={"seq": s, "exp": lax.rem(z + 1, n_exp)}, device_id_type=MESH,
        )

    chip = s // 2
    if n_seq == 8:
        chips = (3 - chip, lax.rem(chip + 2, 4), chip + 1 - 2 * lax.rem(chip, 2))
        peers = [2 * c + k for c in chips for k in range(2)] + [s + 1 - 2 * lax.rem(s, 2)]
    else:
        peers = [lax.rem(s + d, n_seq) for d in range(1, n_seq)]

    own_pos = pl.ds(s * local_len, local_len)
    barrier = pltpu.get_barrier_semaphore()
    for d in range(1, n_exp):
        pl.semaphore_signal(
            barrier, inc=1, device_id={"seq": s, "exp": lax.rem(z + d, n_exp)}, device_id_type=MESH
        )
    for d in range(1, n_seq):
        pl.semaphore_signal(
            barrier, inc=1, device_id={"seq": lax.rem(s + d, n_seq), "exp": z}, device_id_type=MESH
        )
    sources = (q_ref, k_ref, v_ref)
    staged = [
        pltpu.make_async_copy(ref, stage.at[i], stage_sem) for i, ref in enumerate(sources)
    ]
    small = [
        pltpu.make_async_copy(seg_hbm, seg_ref, loc_sem.at[0]),
        pltpu.make_async_copy(gain_hbm, gain_ref, loc_sem.at[1]),
        pltpu.make_async_copy(router_hbm, router_ref, loc_sem.at[2]),
    ]
    locals_ = [
        pltpu.make_async_copy(ref.at[s], qkv.at[i, own_pos], qkv_recv.at[i // 2])
        for i, ref in enumerate(sources)
    ]
    own_ids = pltpu.make_async_copy(ids_hbm, idsbuf.at[z], ids_recv)
    w_copies = [
        pltpu.make_async_copy(w_in_ref, win, w_sem.at[0]),
        pltpu.make_async_copy(w_out_ref, wout, w_sem.at[1]),
    ]
    for c in staged + small + locals_ + [own_ids]:
        c.start()
    arrived(stage, stage_sem).wait_recv()
    pl.semaphore_wait(barrier, n_seq + n_exp - 2)

    for i in range(3):
        for to in peers:
            pltpu.make_async_remote_copy(
                src_ref=stage.at[i, to],
                dst_ref=qkv.at[i, own_pos],
                send_sem=qkv_send,
                recv_sem=qkv_recv.at[i // 2],
                device_id={"seq": to, "exp": z},
                device_id_type=MESH,
            ).start()
    for d in range(1, n_exp):
        pltpu.make_async_remote_copy(
            src_ref=ids_hbm,
            dst_ref=idsbuf.at[z],
            send_sem=ids_send,
            recv_sem=ids_recv,
            device_id={"seq": s, "exp": lax.rem(z + d, n_exp)},
            device_id_type=MESH,
        ).start()
    for c in w_copies:
        c.start()

    for c in small:
        c.wait()
    seg_row = seg_ref[pl.ds(s, 1), :].astype(jnp.float32)
    seg_cols = jnp.broadcast_to(seg_row, (hd, seq_len)).T

    arrived(idsbuf, ids_recv).wait_recv()
    count = per * local_len
    for t in range(TOPK):
        line = jnp.concatenate(
            [idsbuf[e, b, t:t + 1, :] for b in range(seqs) for e in range(n_exp)], axis=1
        ).astype(jnp.float32)
        cols = jnp.broadcast_to(line, (128, line.shape[1])).T
        for g in range(groups):
            partial[t, g] = cols[g * count:(g + 1) * count]

    arrived(qkv.at[pl.ds(0, 2)], qkv_recv.at[0]).wait_recv()
    step = 128
    scale = hd ** (-0.5) * 1.4426950408889634
    for first in range(0, seq_len, step):
        reach = first + step
        scores = lax.dot_general(
            qkv[0, first:reach], qkv[1, :reach], (((1,), (1,)), ((), ())),
            preferred_element_type=jnp.float32,
        )
        qpos = first + lax.broadcasted_iota(jnp.int32, (step, reach), 0)
        kpos = lax.broadcasted_iota(jnp.int32, (step, reach), 1)
        same = jnp.concatenate(
            [seg_cols[first:reach] == seg_row[:, j:j + step] for j in range(0, reach, step)], axis=1
        )
        scores = jnp.where((kpos <= qpos) & same, scores, NEG)
        top = jnp.max(scores, axis=-1, keepdims=True)
        p = jnp.exp2((scores - top) * scale)
        total = jnp.sum(p, axis=-1, keepdims=True)
        probs[first:reach, :reach] = p.astype(jnp.bfloat16)
        inverse[first:reach, :] = jnp.broadcast_to(1.0 / total, (step, hd))
    arrived(qkv.at[2], qkv_recv.at[1]).wait_recv()
    for first in range(0, seq_len, step):
        reach = first + step
        o = jnp.dot(
            probs[first:reach, :reach], qkv[2, :reach], preferred_element_type=jnp.float32
        )
        att[first:reach] = (o * inverse[first:reach]).astype(jnp.bfloat16)

    head = pl.ds(pl.multiple_of(z * hd, hd), hd)
    first_group = s // per
    pltpu.make_async_copy(att.at[own_pos], rows.at[s, :, head], att_recv.at[first_group]).start()
    for to in peers[-1:] + peers[:-1]:
        pltpu.make_async_remote_copy(
            src_ref=att.at[pl.ds(to * local_len, local_len)],
            dst_ref=rows.at[s, :, head],
            send_sem=att_send,
            recv_sem=att_recv.at[first_group],
            device_id={"seq": to, "exp": z},
            device_id_type=MESH,
        ).start()

    def ag_copy(g, owner, to, sem):
        cols = pl.ds(pl.multiple_of(owner * hd, hd), hd)
        there = rows.at[pl.ds(g * per, per), :, cols]
        return pltpu.make_async_remote_copy(
            src_ref=there, dst_ref=there, send_sem=sem, recv_sem=ag_recv.at[g],
            device_id={"seq": s, "exp": to}, device_id_type=MESH,
        )

    for i in range(groups):
        g = lax.rem(first_group + i, groups)
        arrived(rows.at[pl.ds(g * per, per), :, head], att_recv.at[g]).wait_recv()
        for d in range(1, n_exp):
            e = lax.rem(z + d, n_exp)
            @pl.when(~(is_end & (e == far)))
            def _():
                ag_copy(g, z, e, ag_send).start()

    for c in w_copies:
        c.wait()

    def rs_copy(g, d):
        e = lax.rem(z + d, n_exp)
        return pltpu.make_async_remote_copy(
            src_ref=part_out.at[pl.ds(g * per, per), pl.ds(pl.multiple_of(e * tok, tok), tok), :],
            dst_ref=part_in.at[d, pl.ds(g * per, per)],
            send_sem=rs_send,
            recv_sem=rs_recv.at[g],
            device_id={"seq": s, "exp": e},
            device_id_type=MESH,
        )

    def rs_hop(g):
        place = jnp.where(is_end, far, away)
        part = pl.ds(pl.multiple_of(place * tok, tok), tok)
        return pltpu.make_async_remote_copy(
            src_ref=part_out.at[pl.ds(g * per, per), part, :],
            dst_ref=relay_in.at[pl.ds(g * per, per)],
            send_sem=rs_send,
            recv_sem=hop_recv.at[g],
            device_id={"seq": s, "exp": near},
            device_id_type=MESH,
        )

    def pass_on(before):
        earlier = pl.ds(before * per, per)
        rs_hop(before).wait_recv()
        part = pl.ds(pl.multiple_of(away * tok, tok), tok)
        both = own_sum[earlier, part, :] + relay_in[earlier].astype(jnp.float32)
        part_out[earlier, part, :] = both.astype(jnp.bfloat16)
        rs_copy(before, lax.rem(away + n_exp - z, n_exp)).start()

    def gathered(g):
        arrived(rows.at[pl.ds(g * per, per), :, pl.ds(0, width - hd)], ag_recv.at[g]).wait_recv()

    mine = pl.ds(pl.multiple_of(z * tok, tok), tok)

    @pl.loop(0, groups)
    def _(i):
        g = lax.rem(first_group + i, groups)
        members = pl.ds(g * per, per)
        gathered(g)

        @pl.when(is_mid)
        def _():
            ag_copy(g, away, near, far_send).start()

        x = rows[members].reshape(count, width).astype(jnp.float32)
        inv = 1.0 / jnp.sqrt(jnp.mean(x * x, axis=-1, keepdims=True) + 1e-06)
        flat = (x * gain_ref[...]).astype(jnp.bfloat16)
        logits = inv * lax.dot_general(
            flat, router_ref[...], (((1,), (1,)), ((), ())), preferred_element_type=jnp.float32
        )
        total = logits.shape[1]
        names = lax.broadcasted_iota(jnp.int32, logits.shape, 1).astype(jnp.float32)
        id0, id1 = partial[0, g], partial[1, g]
        c0 = jnp.sum(jnp.where(names == id0[:, :total], logits, 0.0), axis=-1, keepdims=True)
        c1 = jnp.sum(jnp.where(names == id1[:, :total], logits, 0.0), axis=-1, keepdims=True)
        s0 = 1.0 / (1.0 + jnp.exp(-c0))
        s1 = 1.0 / (1.0 + jnp.exp(-c1))
        half = 0.5 / (s0 + s1)
        g0 = s0 * half
        g1 = s1 * half
        acc = None
        for j in range(experts_here + AHEAD):
            if j < experts_here:
                name = (z * experts_here + j).astype(jnp.float32)
                gate = jnp.where(id0 == name, g0, 0.0) + jnp.where(id1 == name, g1, 0.0)
                gate = jnp.concatenate([gate * inv] * (CHUNK // gate.shape[1]), axis=1)
                for c in range(0, hidden.shape[2], CHUNK):
                    u = jnp.dot(flat, win[j, :, c:c + CHUNK], preferred_element_type=jnp.float32)
                    scaled = u * gate
                    u = u * inv
                    bent = jnp.tanh(u * (0.7978845608028654 + 0.035677408136300125 * (u * u)))
                    hidden[j, :, c:c + CHUNK] = (scaled + scaled * bent).astype(jnp.bfloat16)
            if j >= AHEAD:
                t = jnp.dot(
                    hidden[j - AHEAD], wout[j - AHEAD], preferred_element_type=jnp.float32
                )
                acc = t if acc is None else acc + t
        acc = acc.reshape(per, local_len, width)
        part_out[members] = acc.astype(jnp.bfloat16)
        own_sum[members] = acc
        direct = i >= RELAYED

        @pl.when(is_end & ~direct)
        def _():
            rs_hop(g).start()

        @pl.when(is_end & direct)
        def _():
            rs_copy(g, lax.rem(far + n_exp - z, n_exp)).start()

        for d in range(1, n_exp):
            e = lax.rem(z + d, n_exp)

            @pl.when(is_end & (e != far) & (i == groups - 1))
            def _():
                rs_copy(lax.rem(g + groups - 1, groups), d).start()

        for d in range(1, n_exp):
            e = lax.rem(z + d, n_exp)
            held = (is_end & ((e == far) | (i == groups - 2))) | (is_mid & ~direct & (e == away))

            @pl.when(~held)
            def _():
                rs_copy(g, d).start()

    @pl.when(is_mid)
    def _():
        for i in range(RELAYED):
            pass_on(lax.rem(first_group + i, groups))

    for i in range(groups):
        g = lax.rem(first_group + i, groups)
        members = pl.ds(g * per, per)
        x = rows[members, mine, :].astype(jnp.float32)
        inv = 1.0 / jnp.sqrt(jnp.mean(x * x, axis=-1, keepdims=True) + 1e-06)
        normed_ref[members] = (x * inv * gain_ref[...]).astype(jnp.bfloat16)
        acc = own_sum[members, mine, :]
        if i >= RELAYED:
            arrived(part_in.at[pl.ds(0, n_exp - 1), members], rs_recv.at[g]).wait_recv()
        else:
            @pl.when(is_end)
            def _():
                lost = lax.rem(z + n_exp - far, n_exp)
                arrived(part_in.at[pl.ds(0, n_exp - 2), members], rs_recv.at[g]).wait_recv()
                part_in[lost, members] = jnp.zeros((per, tok, width), jnp.bfloat16)

            @pl.when(~is_end)
            def _():
                arrived(part_in.at[pl.ds(0, n_exp - 1), members], rs_recv.at[g]).wait_recv()

        for d in range(1, n_exp):
            acc = acc + part_in[d, members].astype(jnp.float32)
        mix_ref[members] = acc.astype(jnp.bfloat16)

    def sent(ref, sem):
        arrived(ref, sem).wait_send()

    sent(qkv.at[:, pl.ds(0, seq_len - local_len)], qkv_send)
    sent(att.at[pl.ds(0, seq_len - local_len)], att_send)
    sent(idsbuf.at[pl.ds(0, n_exp - 1)], ids_send)
    sent(part_out.at[:, pl.ds(0, local_len - tok), :], rs_send)

    @pl.when(is_mid)
    def _():
        sent(rows.at[:, :, pl.ds(0, (n_exp - 1) * hd)], ag_send)
        sent(rows.at[:, :, pl.ds(0, hd)], far_send)

    @pl.when(~is_mid)
    def _():
        sent(rows.at[:, :, pl.ds(0, (n_exp - 2) * hd)], ag_send)


def move_kernel(a_ref, b_ref, to_a, to_b, sems):
    first = pltpu.make_async_copy(a_ref, to_a, sems.at[0])
    second = pltpu.make_async_copy(b_ref, to_b, sems.at[1])
    first.start()
    second.start()
    first.wait()
    second.wait()


def fused_body(n_seq, n_exp, queries, keys, values, seg_ids, norm_gain, router_w, expert_ids, w_in, w_out):
    seqs, local_len, hd = queries.shape
    tok = local_len // n_exp
    per = max(1, 128 // local_len)
    groups = seqs // per
    width = norm_gain.shape[0]
    experts_here, sub, ff = w_in.shape
    seq_len = n_seq * local_len
    ids = expert_ids.reshape(tok, seqs, TOPK).transpose(1, 2, 0)
    bf, f32 = jnp.bfloat16, jnp.float32
    hbm = pl.BlockSpec(memory_space=pltpu.HBM)
    vmem = pl.BlockSpec(memory_space=pltpu.VMEM)
    dma = pltpu.SemaphoreType.DMA
    out = pltpu.VMEM((seqs, tok, width), bf)
    normed, mix = pl.pallas_call(
        functools.partial(fused_kernel, n_seq, n_exp, per),
        out_shape=(out, out),
        in_specs=[hbm] * 9,
        out_specs=(vmem, vmem),
        scratch_shapes=[
            pltpu.VMEM(seg_ids.shape, jnp.int32),
            pltpu.VMEM((1, width), f32),
            pltpu.VMEM(router_w.shape[::-1], bf),
            pltpu.VMEM((3, seqs, local_len, hd), bf),
            pltpu.VMEM((3, seq_len, hd), bf),
            pltpu.VMEM((seq_len, seq_len), bf),
            pltpu.VMEM((seq_len, hd), f32),
            pltpu.VMEM((seq_len, hd), bf),
            pltpu.VMEM((seqs, local_len, width), bf),
            pltpu.VMEM((n_exp, seqs, TOPK, tok), jnp.int32),
            pltpu.VMEM((TOPK, groups, per * local_len, 128), f32),
            pltpu.VMEM((seqs, local_len, width), f32),
            pltpu.VMEM((seqs, local_len, width), bf),
            pltpu.VMEM((n_exp, seqs, tok, width), bf),
            pltpu.VMEM((seqs, tok, width), bf),
            pltpu.VMEM((experts_here, per * local_len, ff), bf),
            pltpu.VMEM((experts_here, sub, ff), bf),
            pltpu.VMEM((experts_here, ff, sub), bf),
            dma((2,)), dma(()), dma((3,)), dma(()), dma(()), dma(()), dma((2,)), dma(()), dma((groups,)),
            dma(()), dma(()), dma((groups,)), dma(()), dma((groups,)), dma((groups,)),
        ],
        compiler_params=pltpu.CompilerParams(
            collective_id=0, has_side_effects=True, vmem_limit_bytes=60 * 1024 * 1024
        ),
    )(queries, keys, values, seg_ids, norm_gain.reshape(1, width), router_w.T, ids, w_in, w_out)
    result = jax.ShapeDtypeStruct((seqs, tok, width), bf)
    return pl.pallas_call(
        move_kernel,
        out_shape=(result, result),
        in_specs=[pl.BlockSpec(memory_space=pl.ANY)] * 2,
        out_specs=(hbm, hbm),
        scratch_shapes=[dma((2,))],
        compiler_params=pltpu.CompilerParams(vmem_limit_bytes=1024 * 1024),
    )(normed, mix)


def whole_body(n_seq, n_exp, *args):
    queries, norm_gain = args[0], args[4]
    seqs, local_len, width = queries.shape
    fits = (
        seqs == n_seq and width == HD and norm_gain.shape[0] == SUB
        and local_len % (16 * n_exp) == 0 and (local_len * n_seq) % 128 == 0
        and seqs % max(1, 128 // local_len) == 0 and n_exp == 4
    )
    return fused_body(n_seq, n_exp, *args) if fits else body(*args)


def solution(mesh):
    return jax.shard_map(
        functools.partial(whole_body, mesh.shape["seq"], mesh.shape["exp"]),
        mesh=mesh,
        in_specs=(
            P(None, "seq", "exp"),
            P(None, "seq", "exp"),
            P(None, "seq", "exp"),
            P(),
            P(),
            P(),
            P(("seq", "exp"), None, None, None),
            P("exp", None, None),
            P("exp", None, None),
        ),
        out_specs=(P(None, ("seq", "exp"), None), P(None, ("seq", "exp"), None)),
        check_vma=False,
    )
```
